32 devices in a mesh: shard: 8 (over z, x), rep: 4 (over y, core).
Axes of the slice: x: 2, y: 2, z: 4, core: 2. Of those that a mesh axis runs over, the one named last changes fastest.
Arguments:
- lender_block: int32 [96, 8], P(('shard', 'rep')), may hold values from 0 to 255, as said below
- confidence: bfloat16 [96, 8, 256, 256], P(('shard', 'rep')), may hold values from 0 to 80, as said below
- lender_factors: bfloat16 [65536, 128], P('shard'), may hold values from -4 to 4
Outputs:
- borrower_factors: float32 [24576, 128], P(('shard', 'rep'))
- lender_rhs: float32 [65536, 128], P('shard')
The draws below stay inside these ranges and needn't reach their ends.
Inputs may be any that keep to these rules, and one draw needn't show every extreme that they name: `lender_block`: within one device's 3 borrower blocks, at most 6 of the 3 x 8 entries name blocks of any one owner (block // 32), and on every device some owner is named exactly 6 times. `confidence`: about half the entries are zero; the others are positive.
All inputs are finite; a program needn't handle non-finite values.
Results may differ from the reference program's by a relative error of at most 0.0047.
Values may be sent and summed in bfloat16 or wider, within the bound.
A program may use at most 128 MiB of HBM per device.

```python
import math
import jax
import jax.numpy as jnp
from jax import lax

R = 128
TILE = 256
K = 8
CG_STEPS = 3
BB = 3
LB_DEV = 32
CAP = 6
BORROW_BLOCKS = 96
LENDER_BLOCKS = 256
BORROWERS = 24576
LENDERS = 65536


def draw_lender_block(key, part):
    devices = BORROW_BLOCKS // BB
    owners_count = LENDER_BLOCKS // LB_DEV
    entries = BB * K
    pool = jnp.repeat(jnp.arange(owners_count, dtype=jnp.int32), CAP)

    def one_device(inner):
        first, second, third, fourth = jax.random.split(inner, 4)
        favoured = jax.random.randint(first, (), 0, owners_count)
        scores = jax.random.permutation(second, owners_count * CAP).astype(jnp.int32)
        scores = jnp.where(pool == favoured, scores - owners_count * CAP, scores)
        order = jnp.argsort(scores)
        owners = pool[order][:entries]
        owners = jax.random.permutation(third, owners)
        within = jax.random.randint(fourth, (entries,), 0, LB_DEV)
        return (owners * LB_DEV + within).reshape(BB, K)
    keys = jax.random.split(jax.random.fold_in(key, 11), devices)
    return jax.vmap(one_device)(keys).reshape(BORROW_BLOCKS, K).astype(jnp.int32)


def draw_confidence(key, part):
    shape = (BORROW_BLOCKS, K, TILE, TILE)
    first, second = jax.random.split(jax.random.fold_in(key, 23))
    seen = jax.random.uniform(first, shape) < 0.5
    base = LENDERS / (K * TILE * 4.0)
    level = jnp.exp(jax.random.uniform(second, shape, maxval=math.log(10.0)))
    return jnp.where(seen, base * level, 0.0).astype(jnp.bfloat16)


def draw_lender_factors(key, part):
    first, second = jax.random.split(jax.random.fold_in(key, 37), 2)
    owners_count = LENDER_BLOCKS // LB_DEV
    rows = jnp.arange(LENDERS)
    owner = (rows // (LB_DEV * TILE)).astype(jnp.float32)
    ramp = jnp.sqrt(1.0 + 2.0 * owner / max(owners_count - 1, 1))
    row_scale = jnp.exp(jax.random.uniform(first, (LENDERS,), maxval=math.log(10.0)))
    values = jnp.clip(jax.random.normal(second, (LENDERS, R)), -4.0, 4.0)
    scaled = values * (row_scale * ramp)[:, None] / (4.6 * math.sqrt(LENDERS))
    return jnp.clip(scaled, -4.0, 4.0).astype(jnp.bfloat16)


def setup_inputs(seed: int = 0) -> dict:
    seeds = jax.random.split(jax.random.key(seed), 4)
    return {
        "lender_block": draw_lender_block(jax.random.fold_in(seeds[3], 71), 0),
        "confidence": draw_confidence(jax.random.fold_in(seeds[3], 71), 0),
        "lender_factors": draw_lender_factors(jax.random.fold_in(seeds[3], 71), 0),
    }


HIGH = lax.Precision.HIGHEST


def apply_system(direction, weights, fetched, gram):
    low = lax.optimization_barrier(direction.astype(jnp.bfloat16)).astype(jnp.float32)
    scores = jnp.einsum("tr,klr->ktl", low, fetched, precision=HIGH)
    weighted = lax.optimization_barrier((weights * scores).astype(jnp.bfloat16)).astype(jnp.float32)
    back = jnp.einsum("ktl,klr->tr", weighted, fetched, precision=HIGH)
    return jnp.dot(direction, gram, precision=HIGH, preferred_element_type=jnp.float32) + 0.1 * direction + back


def reference(lender_block, confidence, lender_factors):
    table = lender_factors.reshape(LENDER_BLOCKS, TILE, R)
    gram = jnp.dot(lender_factors.T, lender_factors, preferred_element_type=jnp.float32)

    def step(total, item):
        block_ids, weights_low = item
        fetched = table[block_ids].astype(jnp.float32)
        weights = weights_low.astype(jnp.float32)
        rhs = jnp.einsum("ktl,klr->tr", weights, fetched, precision=HIGH)
        solution = jnp.zeros((TILE, R), jnp.float32)
        resid = rhs
        direction = rhs
        norm_now = jnp.sum(resid * resid, axis=1, keepdims=True)
        for count in range(CG_STEPS):
            image = apply_system(direction, weights, fetched, gram)
            alpha = norm_now / (jnp.sum(direction * image, axis=1, keepdims=True) + 1e-6)
            solution = solution + alpha * direction
            resid = resid - alpha * image
            norm_next = jnp.sum(resid * resid, axis=1, keepdims=True)
            direction = resid + norm_next / (norm_now + 1e-6) * direction
            norm_now = norm_next
        solved = lax.optimization_barrier(solution.astype(jnp.bfloat16)).astype(jnp.float32)
        partial_rhs = jnp.einsum("ktl,tr->klr", weights, solved, precision=HIGH)
        total = total.at[block_ids.astype(jnp.int32)].add(partial_rhs)
        return total, solution

    start = jnp.zeros((LENDER_BLOCKS, TILE, R), jnp.float32)
    total, solutions = lax.scan(step, start, (lender_block, confidence))
    borrower_factors = solutions.reshape(BORROWERS, R)
    lender_rhs = total.reshape(LENDERS, R) / LENDERS
    return borrower_factors, lender_rhs
```

```python
import jax
import jax.numpy as jnp
from jax import lax
from jax.sharding import PartitionSpec as P

CG_STEPS = 3


HIGH = lax.Precision.HIGHEST


def apply_system(direction, confidence, fetched, gram):
    low = direction.astype(jnp.bfloat16)
    scores = jnp.einsum("btr,bklr->bktl", low, fetched, preferred_element_type=jnp.float32)
    weighted = (confidence.astype(jnp.float32) * scores).astype(jnp.bfloat16)
    back = jnp.einsum("bktl,bklr->btr", weighted, fetched, preferred_element_type=jnp.float32)
    width = direction.shape[-1]
    global_part = jnp.dot(
        direction.reshape(-1, width), gram, precision=HIGH, preferred_element_type=jnp.float32
    )
    return global_part.reshape(direction.shape) + 0.1 * direction + back


WIRE = jnp.float16
TOP = 14.0
EXTRA = 16


def encode(value):
    largest = jnp.maximum(jnp.max(jnp.abs(value)), 1e-30)
    level = jnp.ceil(jnp.log2(largest))
    return (value * jnp.exp2(TOP - level)).astype(WIRE), level


def with_level(chunks, level):
    head = jnp.broadcast_to(level.astype(WIRE), (chunks.shape[0], EXTRA, chunks.shape[2]))
    return jnp.concatenate([chunks, head], axis=1)


def decode(packed, rows):
    level = packed[:, rows : rows + 1, :1].astype(jnp.float32)
    return packed[:, :rows].astype(jnp.float32) * jnp.exp2(level - TOP)


def per_device(lender_block, confidence, lender_factors):
    shards = lax.axis_size("shard")
    blocks, lists = lender_block.shape
    tile = confidence.shape[2]
    rank = lender_factors.shape[1]
    owned = lender_factors.shape[0] // tile
    entries = blocks * lists
    slots = (2 * entries + shards - 1) // shards
    reps = lax.axis_size("rep")
    me = lax.axis_index("shard")
    part = tile // reps
    local_gram = lax.dot_general(
        lender_factors, lender_factors, (((0,), (0,)), ((), ())), preferred_element_type=jnp.float32
    )
    flat = lender_block.reshape(entries)
    listed = lax.all_gather(flat, ("shard", "rep"), axis=0, tiled=False)
    mine = (listed // owned == me).astype(jnp.int32)
    place = jnp.cumsum(mine, axis=1) - 1
    slot_ids = jnp.arange(slots, dtype=jnp.int32)
    hit = (place[:, :, None] == slot_ids) & (mine[:, :, None] == 1)
    within = listed - owned * me
    named = jnp.sum(jnp.where(hit, within[:, :, None] + 1, 0), axis=1) - 1
    owner = flat // owned
    member = (owner[:, None] == jnp.arange(shards, dtype=jnp.int32)[None, :]).astype(jnp.int32)
    position = jnp.sum(jnp.cumsum(member, axis=0) * member, axis=1) - 1
    slot_index = owner * slots + position
    table = lender_factors.reshape(owned, tile, rank)
    incoming = lax.dynamic_index_in_dim(
        named.reshape(shards, reps, slots), lax.axis_index("rep"), axis=1, keepdims=False
    )
    wanted = table[jnp.maximum(incoming, 0)]
    wanted, local_gram = lax.optimization_barrier((wanted, local_gram))
    gram = lax.psum(local_gram, "shard")
    replies = lax.all_to_all(wanted, "shard", split_axis=0, concat_axis=0, tiled=True)
    fetched = replies.reshape(shards * slots, tile, rank)[slot_index].reshape(
        blocks, lists, tile, rank
    )
    rhs = jnp.einsum("bktl,bklr->btr", confidence, fetched, preferred_element_type=jnp.float32)
    solution = jnp.zeros_like(rhs)
    resid = rhs
    direction = rhs
    norm_now = jnp.sum(resid * resid, axis=2, keepdims=True)
    for count in range(CG_STEPS):
        image = apply_system(direction, confidence, fetched, gram)
        alpha = norm_now / (jnp.sum(direction * image, axis=2, keepdims=True) + 1e-06)
        solution = solution + alpha * direction
        resid = resid - alpha * image
        norm_next = jnp.sum(resid * resid, axis=2, keepdims=True)
        direction = resid + norm_next / (norm_now + 1e-06) * direction
        norm_now = norm_next
    solved = solution.astype(jnp.bfloat16)
    partial_rhs = jnp.einsum(
        "bktl,btr->bklr", confidence, solved, preferred_element_type=jnp.float32
    )
    coded, level = encode(partial_rhs)
    every = jnp.arange(shards * slots, dtype=jnp.int32)
    source = jnp.argmax(slot_index[None, :] == every[:, None], axis=1).astype(jnp.int32)
    quarter = jnp.arange(reps, dtype=jnp.int32)
    pick = source.reshape(shards, 1, slots) * reps + quarter[None, :, None]
    chunks = coded.reshape(entries * reps, part, rank)[pick.reshape(-1)]
    chunks = chunks.reshape(shards * reps, slots * part, rank)
    outgoing = with_level(chunks, level)
    returned = lax.all_to_all(outgoing, ("shard", "rep"), split_axis=0, concat_axis=0, tiled=True)
    back = decode(returned, slots * part)
    selector = (
        named.reshape(-1)[None, :] == jnp.arange(owned, dtype=jnp.int32)[:, None]
    ).astype(jnp.float32)
    owner_sum = jnp.dot(
        selector,
        back.reshape(shards * reps * slots, part * rank),
        precision=HIGH,
        preferred_element_type=jnp.float32,
    )
    coded, level = encode(owner_sum.reshape(owned * part, rank))
    shared = lax.all_gather(with_level(coded[None], level)[0], "rep", axis=0, tiled=False)
    lenders_all = owned * tile * shards
    total = decode(shared, owned * part) / lenders_all
    lender_rhs = total.reshape(reps, owned, part, rank).transpose(1, 0, 2, 3)
    lender_rhs = lender_rhs.reshape(owned * tile, rank)
    return (solution.reshape(blocks * tile, rank), lender_rhs)


def solution(mesh):
    in_specs = (P(("shard", "rep"), None), P(("shard", "rep"), None, None, None), P("shard", None))
    out_specs = (P(("shard", "rep"), None), P("shard", None))
    return jax.shard_map(
        per_device, mesh=mesh, in_specs=in_specs, out_specs=out_specs, check_vma=False
    )
```

```python
import jax
import jax.numpy as jnp
from jax import lax
from jax.sharding import PartitionSpec as P

CG_STEPS = 3


HIGH = lax.Precision.HIGHEST


def apply_system(direction, confidence, fetched, gram):
    low = direction.astype(jnp.bfloat16)
    scores = jnp.einsum("btr,bklr->bktl", low, fetched, preferred_element_type=jnp.float32)
    weighted = (confidence.astype(jnp.float32) * scores).astype(jnp.bfloat16)
    back = jnp.einsum("bktl,bklr->btr", weighted, fetched, preferred_element_type=jnp.float32)
    width = direction.shape[-1]
    global_part = jnp.dot(
        direction.reshape(-1, width), gram, precision=HIGH, preferred_element_type=jnp.float32
    )
    return global_part.reshape(direction.shape) + 0.1 * direction + back


WIRE = jnp.float16
TOP = 14.0
EXTRA = 16


def encode(value):
    largest = jnp.maximum(jnp.max(jnp.abs(value)), 1e-30)
    level = jnp.ceil(jnp.log2(largest))
    return (value * jnp.exp2(TOP - level)).astype(WIRE), level


def with_level(chunks, level):
    head = jnp.broadcast_to(level.astype(WIRE), (chunks.shape[0], EXTRA, chunks.shape[2]))
    return jnp.concatenate([chunks, head], axis=1)


def decode(packed, rows):
    level = packed[:, rows : rows + 1, :1].astype(jnp.float32)
    return packed[:, :rows].astype(jnp.float32) * jnp.exp2(level - TOP)


def per_device(lender_block, confidence, lender_factors):
    shards = lax.axis_size("shard")
    blocks, lists = lender_block.shape
    tile = confidence.shape[2]
    rank = lender_factors.shape[1]
    owned = lender_factors.shape[0] // tile
    entries = blocks * lists
    slots = (2 * entries + shards - 1) // shards
    reps = lax.axis_size("rep")
    part = tile // reps
    local_gram = lax.dot_general(
        lender_factors, lender_factors, (((0,), (0,)), ((), ())), preferred_element_type=jnp.float32
    )
    flat = lender_block.reshape(entries)
    owner = flat // owned
    member = (owner[:, None] == jnp.arange(shards, dtype=jnp.int32)[None, :]).astype(jnp.int32)
    position = jnp.sum(jnp.cumsum(member, axis=0) * member, axis=1) - 1
    slot_index = owner * slots + position
    every = jnp.arange(shards * slots, dtype=jnp.int32)
    match = slot_index[None, :] == every[:, None]
    within = flat - owner * owned
    requests = jnp.sum(jnp.where(match, within[None, :] + 1, 0), axis=1) - 1
    requests = jnp.broadcast_to(requests.reshape(shards, 1, slots), (shards, reps, slots))
    named = lax.all_to_all(
        requests.reshape(shards * reps, slots),
        ("shard", "rep"),
        split_axis=0,
        concat_axis=0,
        tiled=True,
    )
    table = lender_factors.reshape(owned, tile, rank)
    incoming = lax.dynamic_index_in_dim(
        named.reshape(shards, reps, slots), lax.axis_index("rep"), axis=1, keepdims=False
    )
    after_gram = (local_gram[0, 0] < 0).astype(jnp.int32)
    wanted = table[jnp.maximum(incoming, 0) + after_gram]
    gram = lax.psum(local_gram, "shard")
    replies = lax.all_to_all(wanted, "shard", split_axis=0, concat_axis=0, tiled=True)
    fetched = replies.reshape(shards * slots, tile, rank)[slot_index].reshape(
        blocks, lists, tile, rank
    )
    rhs = jnp.einsum("bktl,bklr->btr", confidence, fetched, preferred_element_type=jnp.float32)
    solution = jnp.zeros_like(rhs)
    resid = rhs
    direction = rhs
    norm_now = jnp.sum(resid * resid, axis=2, keepdims=True)
    for count in range(CG_STEPS):
        image = apply_system(direction, confidence, fetched, gram)
        alpha = norm_now / (jnp.sum(direction * image, axis=2, keepdims=True) + 1e-06)
        solution = solution + alpha * direction
        resid = resid - alpha * image
        norm_next = jnp.sum(resid * resid, axis=2, keepdims=True)
        direction = resid + norm_next / (norm_now + 1e-06) * direction
        norm_now = norm_next
    solved = solution.astype(jnp.bfloat16)
    partial_rhs = jnp.einsum(
        "bktl,btr->bklr", confidence, solved, preferred_element_type=jnp.float32
    )
    coded, level = encode(partial_rhs)
    source = jnp.argmax(match, axis=1).astype(jnp.int32)
    quarter = jnp.arange(reps, dtype=jnp.int32)
    pick = source.reshape(shards, 1, slots) * reps + quarter[None, :, None]
    chunks = coded.reshape(entries * reps, part, rank)[pick.reshape(-1)]
    chunks = chunks.reshape(shards * reps, slots * part, rank)
    outgoing = with_level(chunks, level)
    returned = lax.all_to_all(outgoing, ("shard", "rep"), split_axis=0, concat_axis=0, tiled=True)
    back = decode(returned, slots * part)
    selector = (
        named.reshape(-1)[None, :] == jnp.arange(owned, dtype=jnp.int32)[:, None]
    ).astype(jnp.float32)
    owner_sum = jnp.dot(
        selector,
        back.reshape(shards * reps * slots, part * rank),
        precision=HIGH,
        preferred_element_type=jnp.float32,
    )
    coded, level = encode(owner_sum.reshape(owned * part, rank))
    shared = lax.all_gather(with_level(coded[None], level)[0], "rep", axis=0, tiled=False)
    lenders_all = owned * tile * shards
    total = decode(shared, owned * part) / lenders_all
    lender_rhs = total.reshape(reps, owned, part, rank).transpose(1, 0, 2, 3)
    lender_rhs = lender_rhs.reshape(owned * tile, rank)
    return (solution.reshape(blocks * tile, rank), lender_rhs)


def solution(mesh):
    in_specs = (P(("shard", "rep"), None), P(("shard", "rep"), None, None, None), P("shard", None))
    out_specs = (P(("shard", "rep"), None), P("shard", None))
    return jax.shard_map(
        per_device, mesh=mesh, in_specs=in_specs, out_specs=out_specs, check_vma=False
    )
```

```python
import jax
import jax.numpy as jnp
from jax import lax
from jax.sharding import PartitionSpec as P

CG_STEPS = 3


HIGH = lax.Precision.HIGHEST


def apply_system(direction, confidence, fetched, gram):
    low = direction.astype(jnp.bfloat16)
    scores = jnp.einsum("btr,bklr->bktl", low, fetched, preferred_element_type=jnp.float32)
    weighted = (confidence.astype(jnp.float32) * scores).astype(jnp.bfloat16)
    back = jnp.einsum("bktl,bklr->btr", weighted, fetched, preferred_element_type=jnp.float32)
    width = direction.shape[-1]
    global_part = jnp.dot(
        direction.reshape(-1, width), gram, precision=HIGH, preferred_element_type=jnp.float32
    )
    return global_part.reshape(direction.shape) + 0.1 * direction + back


WIRE = jnp.float16
TOP = 14.0
EXTRA = 16


def encode(value):
    largest = jnp.maximum(jnp.max(jnp.abs(value)), 1e-30)
    level = jnp.ceil(jnp.log2(largest))
    return (value * jnp.exp2(TOP - level)).astype(WIRE), level


def with_level(chunks, level):
    head = jnp.broadcast_to(level.astype(WIRE), (chunks.shape[0], EXTRA, chunks.shape[2]))
    return jnp.concatenate([chunks, head], axis=1)


def decode(packed, rows):
    level = packed[:, rows : rows + 1, :1].astype(jnp.float32)
    return packed[:, :rows].astype(jnp.float32) * jnp.exp2(level - TOP)


def per_device(lender_block, confidence, lender_factors):
    shards = lax.axis_size("shard")
    blocks, lists = lender_block.shape
    tile = confidence.shape[2]
    rank = lender_factors.shape[1]
    owned = lender_factors.shape[0] // tile
    entries = blocks * lists
    slots = (2 * entries + shards - 1) // shards
    reps = lax.axis_size("rep")
    part = tile // reps
    local_gram = lax.dot_general(
        lender_factors, lender_factors, (((0,), (0,)), ((), ())), preferred_element_type=jnp.float32
    )
    flat = lender_block.reshape(entries)
    owner = flat // owned
    member = (owner[:, None] == jnp.arange(shards, dtype=jnp.int32)[None, :]).astype(jnp.int32)
    position = jnp.sum(jnp.cumsum(member, axis=0) * member, axis=1) - 1
    slot_index = owner * slots + position
    every = jnp.arange(shards * slots, dtype=jnp.int32)
    match = slot_index[None, :] == every[:, None]
    within = flat - owner * owned
    requests = jnp.sum(jnp.where(match, within[None, :] + 1, 0), axis=1) - 1
    requests = jnp.broadcast_to(requests.reshape(shards, 1, slots), (shards, reps, slots))
    named = lax.all_to_all(
        requests.reshape(shards * reps, slots),
        ("shard", "rep"),
        split_axis=0,
        concat_axis=0,
        tiled=True,
    )
    table = lender_factors.reshape(owned, tile, rank)
    incoming = lax.dynamic_index_in_dim(
        named.reshape(shards, reps, slots), lax.axis_index("rep"), axis=1, keepdims=False
    )
    after_gram = (jnp.min(jnp.max(local_gram, axis=1)) < 0).astype(jnp.int32)
    wanted = table[jnp.maximum(incoming, 0) + after_gram]
    gram = lax.psum(local_gram, "shard")
    replies = lax.all_to_all(wanted, "shard", split_axis=0, concat_axis=0, tiled=True)
    fetched = replies.reshape(shards * slots, tile, rank)[slot_index].reshape(
        blocks, lists, tile, rank
    )
    rhs = jnp.einsum("bktl,bklr->btr", confidence, fetched, preferred_element_type=jnp.float32)
    solution = jnp.zeros_like(rhs)
    resid = rhs
    direction = rhs
    norm_now = jnp.sum(resid * resid, axis=2, keepdims=True)
    for count in range(CG_STEPS):
        image = apply_system(direction, confidence, fetched, gram)
        alpha = norm_now / (jnp.sum(direction * image, axis=2, keepdims=True) + 1e-06)
        solution = solution + alpha * direction
        resid = resid - alpha * image
        norm_next = jnp.sum(resid * resid, axis=2, keepdims=True)
        direction = resid + norm_next / (norm_now + 1e-06) * direction
        norm_now = norm_next
    solved = solution.astype(jnp.bfloat16)
    partial_rhs = jnp.einsum(
        "bktl,btr->bklr", confidence, solved, preferred_element_type=jnp.float32
    )
    coded, level = encode(partial_rhs)
    source = jnp.argmax(match, axis=1).astype(jnp.int32)
    quarter = jnp.arange(reps, dtype=jnp.int32)
    pick = source.reshape(shards, 1, slots) * reps + quarter[None, :, None]
    chunks = coded.reshape(entries * reps, part, rank)[pick.reshape(-1)]
    chunks = chunks.reshape(shards * reps, slots * part, rank)
    outgoing = with_level(chunks, level)
    returned = lax.all_to_all(outgoing, ("shard", "rep"), split_axis=0, concat_axis=0, tiled=True)
    back = decode(returned, slots * part)
    selector = (
        named.reshape(-1)[None, :] == jnp.arange(owned, dtype=jnp.int32)[:, None]
    ).astype(jnp.float32)
    owner_sum = jnp.dot(
        selector,
        back.reshape(shards * reps * slots, part * rank),
        precision=HIGH,
        preferred_element_type=jnp.float32,
    )
    coded, level = encode(owner_sum.reshape(owned * part, rank))
    shared = lax.all_gather(with_level(coded[None], level)[0], "rep", axis=0, tiled=False)
    lenders_all = owned * tile * shards
    total = decode(shared, owned * part) / lenders_all
    lender_rhs = total.reshape(reps, owned, part, rank).transpose(1, 0, 2, 3)
    lender_rhs = lender_rhs.reshape(owned * tile, rank)
    return (solution.reshape(blocks * tile, rank), lender_rhs)


def solution(mesh):
    in_specs = (P(("shard", "rep"), None), P(("shard", "rep"), None, None, None), P("shard", None))
    out_specs = (P(("shard", "rep"), None), P("shard", None))
    return jax.shard_map(
        per_device, mesh=mesh, in_specs=in_specs, out_specs=out_specs, check_vma=False
    )
```
